32 devices in a mesh: seq: 8 (over z, core), tp: 4 (over y, x).
Axes of the slice: x: 2, y: 2, z: 4, core: 2. Of those that a mesh axis runs over, the one named last changes fastest.
Arguments:
- hidden_in: bfloat16 [4096, 4608], P('seq'), may hold values from -6 to 6
- pre_gain: float32 [4608], replicated, may hold values from 0.5 to 1.5
- w_query: bfloat16 [4608, 4096], P(None, 'tp'), may hold values from -0.09375 to 0.09375
- key_cache: bfloat16 [8192, 2048], P('seq', 'tp'), may hold values from -12 to 12
- value_cache: bfloat16 [8192, 2048], P('seq', 'tp'), may hold values from -6 to 6
- w_out: bfloat16 [4096, 4608], P('tp'), may hold values from -0.75 to 0.75
- post_gain: float32 [4608], replicated, may hold values from 0.5 to 1.5
- starts: int32 [8], replicated, may hold values from 0 to 7680, as said below
- counts: int32 [8], replicated, may hold values from 512 to 1024, as said below
Outputs:
- layer_out: bfloat16 [4096, 4608], P(('seq', 'tp'))
The draws below stay inside these ranges and needn't reach their ends.
Inputs may be any that keep to these rules, and one draw needn't show every extreme that they name: The queries of shard s sit at positions starts[s] to starts[s] + 511, all inside the filled rows of shard s, that is from s * 1024 to s * 1024 + counts[s] - 1. `counts`: at least one shard is full.
All inputs are finite; a program needn't handle non-finite values.
Results may differ from the reference program's by a relative error of at most 0.012.
Values may be sent and summed in bfloat16 or wider, within the bound.
A program may use at most 128 MiB of HBM per device.

```python
import jax
import jax.numpy as jnp
from jax import lax

D = 4608
H = 32
KVH = 16
HD = 128
WINDOW = 4096
CTX_DEV = 1024
Q_DEV = 512
HALO = 4
CONTEXT = 8192
TOKENS = 4096
N_SEQ = 8
N_TP = 4


def fill_table(key):
    count_key = jax.random.fold_in(key, 11)
    full_key = jax.random.fold_in(key, 12)
    offset_key = jax.random.fold_in(key, 13)
    shard_ids = jnp.arange(N_SEQ, dtype=jnp.int32)
    counts = jax.random.randint(count_key, (N_SEQ,), Q_DEV, CTX_DEV + 1, dtype=jnp.int32)
    full_shard = jax.random.randint(full_key, (), 0, N_SEQ, dtype=jnp.int32)
    counts = jnp.where(shard_ids == full_shard, jnp.int32(CTX_DEV), counts)
    offsets = jax.random.randint(offset_key, (N_SEQ,), 0, counts - Q_DEV + 1, dtype=jnp.int32)
    starts = shard_ids * CTX_DEV + offsets
    return (starts.astype(jnp.int32), counts.astype(jnp.int32))


def draw_starts(key, part):
    return fill_table(key)[0]


def draw_counts(key, part):
    return fill_table(key)[1]


def levels(rng, shape, shards, least, top_value):
    def one(axis_at, blocks):
        draws = jax.random.uniform(jax.random.fold_in(jax.random.fold_in(rng, 6), axis_at), (blocks,), jnp.float32, least / len(shards), top_value / len(shards))
        return jnp.repeat(jnp.exp(draws), shape[axis_at] // blocks).reshape((-1,) + (1,) * (len(shape) - axis_at - 1))

    level = one(*shards[0])
    for cut in shards[1:]:
        level = level * one(*cut)
    return level


def gaussian(key, shape, scale, reach, shards=(), kind=jnp.bfloat16):
    gain = levels(key, shape, shards, -0.22, 0.18) if shards else 1.0
    result = jax.random.normal(key, shape, jnp.float32) * scale * gain
    return jnp.minimum(jnp.maximum(result, -reach), reach).astype(kind)


def setup_inputs(seed: int = 0) -> dict:
    seeds = jax.random.split(jax.random.key(seed), 10)
    hidden_in = gaussian(seeds[0], (TOKENS, D), 1.0, 6.0, ((0, 8),))
    pre_gain = jnp.clip(1.0 + 0.1 * jax.random.normal(seeds[1], (D,), jnp.float32), 0.5, 1.5)
    w_query = gaussian(seeds[2], (D, H * HD), D ** -0.5, 0.09375, ((1, 4),))
    key_cache = gaussian(seeds[3], (CONTEXT, KVH * HD), 2.0, 12.0, ((0, 8), (1, 4)))
    value_cache = gaussian(seeds[4], (CONTEXT, KVH * HD), 1.0, 6.0, ((0, 8), (1, 4)))
    w_out = gaussian(seeds[5], (H * HD, D), (H * HD // 64) ** -0.5, 0.75, ((0, 4),))
    post_gain = jnp.clip(1.0 + 0.1 * jax.random.normal(seeds[6], (D,), jnp.float32), 0.5, 1.5)
    starts = draw_starts(jax.random.fold_in(seeds[9], 71), 0)
    counts = draw_counts(jax.random.fold_in(seeds[9], 71), 0)
    return dict(hidden_in=hidden_in, pre_gain=pre_gain, w_query=w_query, key_cache=key_cache, value_cache=value_cache, w_out=w_out, post_gain=post_gain, starts=starts, counts=counts)


def reference(hidden_in, pre_gain, w_query, key_cache, value_cache, w_out, post_gain, starts, counts):
    per_group = H // KVH
    key_span = (HALO + 1) * CTX_DEV
    inputs = hidden_in.astype(jnp.float32)
    normed = (inputs * lax.rsqrt(lax.optimization_barrier(jnp.mean(inputs * inputs, axis=-1, keepdims=True)) + 0.1) * pre_gain).astype(jnp.bfloat16)
    queries = (jnp.dot(normed, w_query, preferred_element_type=jnp.float32) * (D // H) ** (-0.5)).astype(jnp.bfloat16)
    padding = jnp.zeros((HALO * CTX_DEV, KVH * HD), jnp.bfloat16)
    keys_padded = jnp.concatenate([padding, key_cache], axis=0)
    values_padded = jnp.concatenate([padding, value_cache], axis=0)
    w_groups = w_out.astype(jnp.float32).reshape(N_TP, H * HD // N_TP, D)

    def one_shard(shard):
        shard = shard.astype(jnp.int32)
        query_block = lax.dynamic_slice_in_dim(queries, (shard * Q_DEV).astype(jnp.int32), Q_DEV, 0)
        key_block = lax.dynamic_slice_in_dim(keys_padded, (shard * CTX_DEV).astype(jnp.int32), key_span, 0)
        value_block = lax.dynamic_slice_in_dim(values_padded, (shard * CTX_DEV).astype(jnp.int32), key_span, 0)
        key_pos = (shard - HALO) * CTX_DEV + jnp.arange(key_span, dtype=jnp.int32)
        source = jnp.clip(key_pos // CTX_DEV, 0, N_SEQ - 1).astype(jnp.int32)
        filled = (key_pos >= 0) & (key_pos - source * CTX_DEV < counts[source])
        query_pos = starts[shard] + jnp.arange(Q_DEV, dtype=jnp.int32)
        allowed = filled[None, :] & (key_pos[None, :] <= query_pos[:, None]) & (key_pos[None, :] > query_pos[:, None] - WINDOW)
        query_f = lax.optimization_barrier(query_block).astype(jnp.float32).reshape(Q_DEV, KVH, per_group, HD)
        key_f = key_block.astype(jnp.float32).reshape(key_span, KVH, HD)
        value_f = value_block.astype(jnp.float32).reshape(key_span, KVH, HD)
        scores = jnp.einsum('qkgd,ckd->kgqc', query_f, key_f, precision=lax.Precision.HIGHEST)
        scores = 50.0 * jnp.tanh(scores / 50.0)
        weight = jnp.where(allowed[None, None], jnp.exp(scores), jnp.float32(0.0))
        denominator = lax.optimization_barrier(jnp.sum(weight, axis=-1))
        weight16 = lax.optimization_barrier(weight.astype(jnp.bfloat16)).astype(jnp.float32)
        context = jnp.einsum('kgqc,ckd->qkgd', weight16, value_f, precision=lax.Precision.HIGHEST)
        attended = (context / jnp.transpose(denominator, (2, 0, 1))[..., None]).reshape(Q_DEV, H * HD).astype(jnp.bfloat16)
        attended_f = lax.optimization_barrier(attended).astype(jnp.float32).reshape(Q_DEV, N_TP, H * HD // N_TP)
        partial_value = jnp.einsum('qtf,tfd->tqd', attended_f, w_groups, precision=lax.Precision.HIGHEST)
        partial_value = lax.optimization_barrier(partial_value.astype(jnp.bfloat16)).astype(jnp.float32)
        projected = lax.optimization_barrier(jnp.sum(partial_value, axis=0))
        residual = lax.dynamic_slice_in_dim(hidden_in, (shard * Q_DEV).astype(jnp.int32), Q_DEV, 0).astype(jnp.float32)
        mixed = residual + projected * lax.rsqrt(lax.optimization_barrier(jnp.mean(projected * projected, axis=-1, keepdims=True)) + 0.1) * post_gain
        return mixed.astype(jnp.bfloat16)
    layer_out = lax.map(one_shard, jnp.arange(N_SEQ, dtype=jnp.int32))
    return layer_out.reshape(N_SEQ * Q_DEV, D)
```

```python
import functools
import math

import jax
import jax.numpy as jnp
from jax import lax
from jax.experimental import pallas as pl
from jax.experimental.pallas import tpu as pltpu
from jax.sharding import PartitionSpec as P

HEADS = 32
HD = 128
WINDOW = 4096
NC = 4
QT = 256
NT = 512
SOFT = 50.0
GAIN = SOFT * math.log2(math.e)
MESH = pl.DeviceIdType.MESH
F32 = jnp.float32
BF16 = jnp.bfloat16


def kernel(
    n, n_tp, kvh,
    starts, counts, hidden, pre_gain, wq, key, value, wout, post_gain, out,
    hbuf, wqb, wob, k0, v0, k2, v2, k1, v1, qo, qr, vx, ao, ar, psend, precv,
    proj, rrecv, res, obuf, att,
    hsem, wqsem, wosem, kvsem, ressem, osem,
    s2, r2, s1, r1, sq, rq, sp, rp, ss, rs,
):
    s = lax.axis_index("seq")
    t = lax.axis_index("tp")
    odd = lax.rem(s, 2)
    partner = s + 1 - 2 * odd
    rows, d = hidden.shape
    ctx = key.shape[0]
    sub = rows // (NC * n_tp)
    chunk = rows // NC
    owned = rows // n_tp
    has_prev = s >= 2
    has_next = s + 2 < n

    hcopies = []
    for c in range(NC):
        for b in range(n_tp):
            cp = pltpu.make_async_copy(
                hidden.at[pl.ds(b * owned + c * sub, sub)], hbuf.at[c, b], hsem.at[c, b])
            cp.start()
            hcopies.append(cp)

    def wq_copy(h):
        return pltpu.make_async_copy(
            wq.at[:, pl.ds(pl.multiple_of(h * 2 * HD, 2 * HD), 2 * HD)], wqb.at[h], wqsem.at[h])

    for h in range(kvh):
        wq_copy(h).start()

    barrier = pltpu.get_barrier_semaphore()
    pl.semaphore_signal(barrier, inc=1, device_id=(partner, t), device_id_type=MESH)
    for k in range(1, n_tp):
        pl.semaphore_signal(barrier, inc=1, device_id=(s, lax.rem(t + k, n_tp)), device_id_type=MESH)

    @pl.when(has_prev)
    def _():
        pl.semaphore_signal(barrier, inc=1, device_id=(s - 2, t), device_id_type=MESH)

    @pl.when(has_next)
    def _():
        pl.semaphore_signal(barrier, inc=1, device_id=(s + 2, t), device_id_type=MESH)

    pl.semaphore_wait(
        barrier, n_tp + jnp.where(has_prev, 1, 0) + jnp.where(has_next, 1, 0))

    def cols(h):
        return pl.ds(pl.multiple_of(h * HD, HD), HD)

    def kv_next(h):
        return [
            pltpu.make_async_remote_copy(
                src.at[:, cols(h)], dst.at[h], s2.at[h, j], r2.at[h, j],
                device_id=(s + 2, t), device_id_type=MESH)
            for j, (src, dst) in enumerate(((key, k2), (value, v2)))
        ]

    def kv_own_partner(h):
        return [
            pltpu.make_async_remote_copy(
                src.at[:, cols(h)], dst.at[h], s1.at[h, j], r1.at[h, j],
                device_id=(partner, t), device_id_type=MESH)
            for j, (src, dst) in enumerate(((key, k1), (value, v1)))
        ]

    def kv_relay(h):
        return [
            pltpu.make_async_remote_copy(
                src.at[h], dst.at[h], s1.at[h, j], r1.at[h, j],
                device_id=(partner, t), device_id_type=MESH)
            for j, (src, dst) in enumerate(((k2, k1), (v2, v1)))
        ]

    def q_back(h):
        return pltpu.make_async_remote_copy(
            qo.at[h], qr.at[h], sq.at[h], rq.at[h], device_id=(s - 2, t), device_id_type=MESH)

    def part_next(c):
        return pltpu.make_async_remote_copy(
            psend.at[c], precv.at[c], sp.at[c], rp.at[c],
            device_id=(s + 2, t), device_id_type=MESH)

    def scatter(c, k):
        to = lax.rem(t + k, n_tp)
        return pltpu.make_async_remote_copy(
            proj.at[c, to], rrecv.at[c, k - 1], ss.at[c, k - 1], rs.at[c, k - 1],
            device_id=(s, to), device_id_type=MESH)

    @pl.when(has_next)
    def _():
        for h in range(kvh):
            for cp in kv_next(h):
                cp.start()

    @pl.when(odd == 0)
    def _():
        for h in range(kvh):
            for cp in kv_own_partner(h):
                cp.start()

    def kv_local(h):
        return [
            pltpu.make_async_copy(src.at[:, cols(h)], dst.at[h], kvsem.at[h, j])
            for j, (src, dst) in enumerate(((key, k0), (value, v0)))
        ]

    for h in range(kvh):
        for cp in kv_local(h):
            cp.start()
    wo_copy = pltpu.make_async_copy(wout, wob, wosem)
    wo_copy.start()
    res_copy = pltpu.make_async_copy(
        hidden.at[pl.ds(pl.multiple_of(t * owned, owned), owned)], res, ressem)
    res_copy.start()

    for cp in hcopies:
        cp.wait()

    def norm(i, carry):
        c = i // n_tp
        b = i % n_tp
        x = hbuf[c, b].astype(F32)
        y = x * lax.rsqrt(jnp.mean(x * x, axis=-1, keepdims=True) + 0.1) * pre_gain[...]
        hbuf[c, b] = y.astype(BF16)
        return carry

    lax.fori_loop(0, NC * n_tp, norm, 0)

    def project(h, carry):
        wq_copy(h).wait()
        x = hbuf[...].reshape(rows, d)
        y = jnp.dot(x, wqb[h], preferred_element_type=F32) * ((d // HEADS) ** -0.5 / SOFT)
        y = y.astype(BF16)
        qo[h, 0:rows] = y[:, :HD]
        qo[h, rows:2 * rows] = y[:, HD:]

        @pl.when(has_prev)
        def _():
            q_back(h).start()

        return carry

    lax.fori_loop(0, kvh, project, 0)

    def extend(v, h, filled):
        r = lax.broadcasted_iota(jnp.int32, (ctx, HD), 0)
        ok = r < filled
        vx[:, 0:HD] = jnp.where(ok, v[h].astype(F32), 0.0).astype(BF16)
        vx[:, HD:] = jnp.where(ok, 1.0, 0.0).astype(BF16)

    def unit(q, k, h, acc, first, mode, offset):
        per = QT // chunk

        def tile(i, carry):
            span = pl.ds(pl.multiple_of(i * QT, QT), QT)
            qt = q[h, span]
            ps = []
            kb = 256
            if mode:
                shape = (per, n_tp, sub, kb)
                c0 = lax.rem(i * per, NC)
                pos = (
                    (c0 + lax.broadcasted_iota(jnp.int32, shape, 0)) * sub
                    + lax.broadcasted_iota(jnp.int32, shape, 1) * owned
                    + lax.broadcasted_iota(jnp.int32, shape, 2)
                )
                rel = (lax.broadcasted_iota(jnp.int32, shape, 3) - pos - offset).reshape(QT, kb)
            for b in range(ctx // kb):
                sc = lax.dot_general(
                    qt, k[h, b * kb:(b + 1) * kb], (((1,), (1,)), ((), ())),
                    preferred_element_type=F32)
                p = jnp.exp2(jnp.tanh(sc) * GAIN)
                if mode == 1:
                    p = jnp.where(rel <= -b * kb, p, 0.0)
                elif mode == 2:
                    p = jnp.where(rel > -b * kb, p, 0.0)
                ps.append(p.astype(BF16))
            a = jnp.dot(jnp.concatenate(ps, axis=1), vx[...], preferred_element_type=F32)
            if first:
                acc[h, span] = a
            else:
                acc[h, span] += a
            return carry

        lax.fori_loop(0, 2 * rows // QT, tile, 0, unroll=2)

    off_own = starts[s] - s * ctx
    s_next = jnp.minimum(s + 2, n - 1)
    off_next = starts[s_next] - s_next * ctx + (2 + 2) * ctx - WINDOW
    fill1 = counts[jnp.maximum(s - 1, 0)]
    fill2 = counts[jnp.maximum(s - 2, 0)]

    def own(h, carry):
        for cp in kv_local(h):
            cp.wait()
        extend(v0, h, ctx)
        unit(qo, k0, h, ao, True, 1, off_own)
        ar[h] = jnp.zeros_like(ar[h])
        return carry

    lax.fori_loop(0, kvh, own, 0)

    def far(h, carry):
        @pl.when(has_prev)
        def _():
            for cp in kv_next(h):
                cp.wait_recv()

        @pl.when(has_prev & (odd == 1))
        def _():
            for cp in kv_relay(h):
                cp.start()

        @pl.when(has_next)
        def _():
            q_back(h).wait_recv()

        @pl.when(has_prev)
        def _():
            extend(v2, h, fill2)
            unit(qo, k2, h, ao, False, 0, 0)

            @pl.when(has_next)
            def _():
                unit(qr, k2, h, ar, False, 2, off_next)

        @pl.when(s >= 1)
        def _():
            @pl.when(has_prev | (odd == 1))
            def _():
                for cp in kv_own_partner(h):
                    cp.wait_recv()

            extend(v1, h, fill1)
            unit(qo, k1, h, ao, False, 0, 0)

            @pl.when(has_next)
            def _():
                unit(qr, k1, h, ar, False, 0, 0)

        return carry

    lax.fori_loop(0, kvh, far, 0)

    lane = lax.broadcasted_iota(jnp.int32, (chunk, HD), 1)
    heads = 2 * kvh

    @pl.when(has_next)
    def _():
        for c in range(NC):
            pack = jnp.zeros((chunk, HD), F32)
            for h in range(kvh):
                for g in range(2):
                    r0 = g * rows + c * chunk
                    j = 2 * h + g
                    psend[c, j] = ar[h, r0:r0 + chunk, 0:HD].astype(BF16)
                    den = ar[h, r0:r0 + chunk, HD:2 * HD]
                    hi = den.astype(BF16).astype(F32)
                    pack = jnp.where(lane == j, hi, pack)
                    pack = jnp.where(lane == heads + j, den - hi, pack)
            psend[c, heads] = pack.astype(BF16)
            part_next(c).start()

    wo_copy.wait()

    @pl.when(s < 2)
    def _():
        precv[...] = jnp.zeros_like(precv)

    def finish(c, carry):
        @pl.when(has_prev)
        def _():
            part_next(c).wait_recv()

        pack = precv[c, heads].astype(F32)
        for h in range(kvh):
            for g in range(2):
                j = 2 * h + g
                span = pl.ds(pl.multiple_of(g * rows + c * chunk, chunk), chunk)
                den = (
                    ao[h, span, HD:2 * HD]
                    + pack[:, j:j + 1] + pack[:, heads + j:heads + j + 1]
                )
                num = ao[h, span, 0:HD] + precv[c, j].astype(F32)
                att[:, j * HD:(j + 1) * HD] = (num / den).astype(BF16)

        def column(i, inner):
            cs = pl.ds(pl.multiple_of(i * NT, NT), NT)
            y = jnp.dot(att[...], wob[:, cs], preferred_element_type=F32).astype(BF16)
            proj[c, :, :, cs] = y.reshape(n_tp, sub, NT)
            return inner

        lax.fori_loop(0, d // NT, column, 0)
        for k in range(1, n_tp):
            scatter(c, k).start()
        return carry

    lax.fori_loop(0, NC, finish, 0)
    res_copy.wait()

    def out_copy(c):
        return pltpu.make_async_copy(
            obuf.at[c], out.at[pl.ds(pl.multiple_of(c * sub, sub), sub)], osem.at[c])

    def close(c, carry):
        total = proj[c, t].astype(F32)
        for k in range(1, n_tp):
            scatter(c, k).wait_recv()
            total += rrecv[c, k - 1].astype(F32)
        scale = lax.rsqrt(jnp.mean(total * total, axis=-1, keepdims=True) + 0.1)
        r = res[pl.ds(pl.multiple_of(c * sub, sub), sub)].astype(F32)
        obuf[c] = (r + total * scale * post_gain[...]).astype(BF16)
        out_copy(c).start()
        return carry

    lax.fori_loop(0, NC, close, 0)

    def drain(h, carry):
        @pl.when(has_next)
        def _():
            for cp in kv_next(h):
                cp.wait_send()

        @pl.when(odd == 0)
        def _():
            for cp in kv_own_partner(h):
                cp.wait_send()

        @pl.when(has_prev & (odd == 1))
        def _():
            for cp in kv_relay(h):
                cp.wait_send()

        @pl.when(has_prev)
        def _():
            q_back(h).wait_send()

        return carry

    lax.fori_loop(0, kvh, drain, 0)

    def drain_chunks(c, carry):
        @pl.when(has_next)
        def _():
            part_next(c).wait_send()

        for k in range(1, n_tp):
            scatter(c, k).wait_send()
        out_copy(c).wait()
        return carry

    lax.fori_loop(0, NC, drain_chunks, 0)


def shards(n, n_tp, hidden_in, pre_gain, w_query, key_cache, value_cache, w_out, post_gain, starts, counts):
    rows, d = hidden_in.shape
    ctx, kvw = key_cache.shape
    kvh = kvw // HD
    sub = rows // (NC * n_tp)
    chunk = rows // NC
    dma = pltpu.SemaphoreType.DMA
    kv = pltpu.VMEM((kvh, ctx, HD), BF16)
    any_spec = pl.BlockSpec(memory_space=pl.ANY)
    vmem_spec = pl.BlockSpec(memory_space=pltpu.VMEM)
    smem_spec = pl.BlockSpec(memory_space=pltpu.SMEM)
    return pl.pallas_call(
        functools.partial(kernel, n, n_tp, kvh),
        out_shape=jax.ShapeDtypeStruct((rows // n_tp, d), BF16),
        in_specs=[smem_spec, smem_spec, any_spec, vmem_spec] + [any_spec] * 4 + [vmem_spec],
        out_specs=any_spec,
        scratch_shapes=[
            pltpu.VMEM((NC, n_tp, sub, d), BF16),
            pltpu.VMEM((kvh, d, 2 * HD), BF16),
            pltpu.VMEM(w_out.shape, BF16),
            kv, kv, kv, kv, kv, kv,
            pltpu.VMEM((kvh, 2 * rows, HD), BF16),
            pltpu.VMEM((kvh, 2 * rows, HD), BF16),
            pltpu.VMEM((ctx, 2 * HD), BF16),
            pltpu.VMEM((kvh, 2 * rows, 2 * HD), F32),
            pltpu.VMEM((kvh, 2 * rows, 2 * HD), F32),
            pltpu.VMEM((NC, 2 * kvh + 1, chunk, HD), BF16),
            pltpu.VMEM((NC, 2 * kvh + 1, chunk, HD), BF16),
            pltpu.VMEM((NC, n_tp, sub, d), BF16),
            pltpu.VMEM((NC, n_tp - 1, sub, d), BF16),
            pltpu.VMEM((rows // n_tp, d), BF16),
            pltpu.VMEM((NC, sub, d), BF16),
            pltpu.VMEM((chunk, w_out.shape[0]), BF16),
            dma((NC, n_tp)), dma((kvh,)), dma, dma((kvh, 2)), dma, dma((NC,)),
            dma((kvh, 2)), dma((kvh, 2)), dma((kvh, 2)), dma((kvh, 2)),
            dma((kvh,)), dma((kvh,)), dma((NC,)), dma((NC,)),
            dma((NC, n_tp - 1)), dma((NC, n_tp - 1)),
        ],
        compiler_params=pltpu.CompilerParams(
            collective_id=0, has_side_effects=True, vmem_limit_bytes=67_000_000),
        name="attention_block",
    )(starts, counts, hidden_in, pre_gain.reshape(1, d), w_query, key_cache, value_cache, w_out,
      post_gain.reshape(1, d))


def solution(mesh):
    return jax.shard_map(
        functools.partial(shards, mesh.shape["seq"], mesh.shape["tp"]),
        mesh=mesh,
        in_specs=(
            P("seq", None),
            P(),
            P(None, "tp"),
            P("seq", "tp"),
            P("seq", "tp"),
            P("tp", None),
            P(),
            P(),
            P(),
        ),
        out_specs=P(("seq", "tp"), None),
        check_vma=False,
    )
```

```python
import functools
import math

import jax
import jax.numpy as jnp
from jax import lax
from jax.experimental import pallas as pl
from jax.experimental.pallas import tpu as pltpu
from jax.sharding import PartitionSpec as P

HEADS = 32
HD = 128
WINDOW = 4096
SUB = 32
QT = 256
NT = 256
SOFT = 50.0
GAIN = SOFT * math.log2(math.e)
MESH = pl.DeviceIdType.MESH
F32 = jnp.float32
BF16 = jnp.bfloat16


def kernel(
    n, n_tp, kvh, NC,
    starts, counts, hidden, pre_gain, wq, key, value, wout, post_gain, out,
    hbuf, wqb, wob, k0, v0, k2, v2, k1, v1, qo, qr, vx0, vx1, vx2, ao, ar, psend, precv,
    proj, ra1, pa, ra2, rb1, pb, rb2, res, obuf, att,
    hsem, wqsem, wosem, kvsem, ressem, osem,
    s2, r2, s1, r1, sq, rq, sp, rp,
    sa1, ta1, sa2, ta2, sb1, tb1, sb2, tb2,
):
    s = lax.axis_index("seq")
    t = lax.axis_index("tp")
    odd = lax.rem(s, 2)
    partner = s + 1 - 2 * odd
    rows, d = hidden.shape
    ctx = key.shape[0]
    sub = rows // (NC * n_tp)
    chunk = rows // NC
    owned = rows // n_tp
    has_prev = s >= 2
    has_next = s + 2 < n

    hcopies = []
    for c in range(NC):
        for b in range(n_tp):
            cp = pltpu.make_async_copy(
                hidden.at[pl.ds(b * owned + c * sub, sub)], hbuf.at[c, b], hsem.at[c, b])
            cp.start()
            hcopies.append(cp)

    def wq_copy(h):
        return pltpu.make_async_copy(
            wq.at[:, pl.ds(pl.multiple_of(h * 2 * HD, 2 * HD), 2 * HD)], wqb.at[h], wqsem.at[h])

    for h in range(kvh):
        wq_copy(h).start()

    barrier = pltpu.get_barrier_semaphore()
    pl.semaphore_signal(barrier, inc=1, device_id=(partner, t), device_id_type=MESH)
    for k in range(1, n_tp):
        pl.semaphore_signal(barrier, inc=1, device_id=(s, lax.rem(t + k, n_tp)), device_id_type=MESH)

    @pl.when(has_prev)
    def _():
        pl.semaphore_signal(barrier, inc=1, device_id=(s - 2, t), device_id_type=MESH)

    @pl.when(has_next)
    def _():
        pl.semaphore_signal(barrier, inc=1, device_id=(s + 2, t), device_id_type=MESH)

    pl.semaphore_wait(
        barrier, n_tp + jnp.where(has_prev, 1, 0) + jnp.where(has_next, 1, 0))

    def cols(h):
        return pl.ds(pl.multiple_of(h * HD, HD), HD)

    def kv_next(h):
        return [
            pltpu.make_async_remote_copy(
                src.at[:, cols(h)], dst.at[h], s2.at[h, j], r2.at[h, j],
                device_id=(s + 2, t), device_id_type=MESH)
            for j, (src, dst) in enumerate(((key, k2), (value, v2)))
        ]

    def kv_own_partner(h):
        return [
            pltpu.make_async_remote_copy(
                src.at[:, cols(h)], dst.at[h], s1.at[h, j], r1.at[h, j],
                device_id=(partner, t), device_id_type=MESH)
            for j, (src, dst) in enumerate(((key, k1), (value, v1)))
        ]

    def kv_relay(h):
        return [
            pltpu.make_async_remote_copy(
                src.at[h], dst.at[h], s1.at[h, j], r1.at[h, j],
                device_id=(partner, t), device_id_type=MESH)
            for j, (src, dst) in enumerate(((k2, k1), (v2, v1)))
        ]

    def q_back(h):
        return pltpu.make_async_remote_copy(
            qo.at[h], qr.at[h], sq.at[h], rq.at[h], device_id=(s - 2, t), device_id_type=MESH)

    def part_next(c):
        return pltpu.make_async_remote_copy(
            psend.at[c], precv.at[c], sp.at[c], rp.at[c],
            device_id=(s + 2, t), device_id_type=MESH)

    nx = 2
    ny = n_tp // nx
    half = d // 2
    x_own = lax.rem(t, nx)
    y_own = lax.div(t, nx)
    left = pl.ds(0, half)
    right = pl.ds(half, half)

    def remote(src, dst, send, recv, to):
        return pltpu.make_async_remote_copy(
            src, dst, send, recv, device_id=(s, to), device_id_type=MESH)

    def first_phase(c):
        copies = []
        for k in range(1, nx):
            xt = lax.rem(x_own + k, nx)
            copies.append(remote(
                proj.at[c, :, xt, :, left], ra1.at[c, k - 1], sa1.at[c, k - 1], ta1.at[c, k - 1],
                y_own * nx + xt))
        for k in range(1, ny):
            yt = lax.rem(y_own + k, ny)
            copies.append(remote(
                proj.at[c, yt, :, :, right], rb1.at[c, k - 1], sb1.at[c, k - 1], tb1.at[c, k - 1],
                yt * nx + x_own))
        return copies

    def second_phase(c):
        copies = []
        for k in range(1, ny):
            yt = lax.rem(y_own + k, ny)
            copies.append(remote(
                pa.at[c, yt], ra2.at[c, k - 1], sa2.at[c, k - 1], ta2.at[c, k - 1],
                yt * nx + x_own))
        for k in range(1, nx):
            xt = lax.rem(x_own + k, nx)
            copies.append(remote(
                pb.at[c, xt], rb2.at[c, k - 1], sb2.at[c, k - 1], tb2.at[c, k - 1],
                y_own * nx + xt))
        return copies

    @pl.when(has_next)
    def _():
        for h in range(kvh):
            for cp in kv_next(h):
                cp.start()

    @pl.when(odd == 0)
    def _():
        for h in range(kvh):
            for cp in kv_own_partner(h):
                cp.start()

    def kv_local(h):
        return [
            pltpu.make_async_copy(src.at[:, cols(h)], dst.at[h], kvsem.at[h, j])
            for j, (src, dst) in enumerate(((key, k0), (value, v0)))
        ]

    for h in range(kvh):
        for cp in kv_local(h):
            cp.start()
    wo_copy = pltpu.make_async_copy(wout, wob, wosem)
    wo_copy.start()
    res_copy = pltpu.make_async_copy(
        hidden.at[pl.ds(pl.multiple_of(t * owned, owned), owned)], res, ressem)
    res_copy.start()

    for cp in hcopies:
        cp.wait()

    def norm(i, carry):
        c = i // n_tp
        b = i % n_tp
        x = hbuf[c, b].astype(F32)
        y = x * lax.rsqrt(jnp.mean(x * x, axis=-1, keepdims=True) + 0.1) * pre_gain[...]
        hbuf[c, b] = y.astype(BF16)
        return carry

    lax.fori_loop(0, NC * n_tp, norm, 0)

    def project(h, carry):
        wq_copy(h).wait()
        x = hbuf[...].reshape(rows, d)
        y = jnp.dot(x, wqb[h], preferred_element_type=F32) * ((d // HEADS) ** -0.5 / SOFT)
        y = y.astype(BF16)
        qo[h, 0:rows] = y[:, :HD]
        qo[h, rows:2 * rows] = y[:, HD:]

        @pl.when(has_prev)
        def _():
            q_back(h).start()

        return carry

    lax.fori_loop(0, kvh, project, 0)

    def extend(vx, v, h, filled):
        r = lax.broadcasted_iota(jnp.int32, (ctx, HD), 0)
        ok = r < filled
        vx[:, 0:HD] = jnp.where(ok, v[h].astype(F32), 0.0).astype(BF16)
        vx[:, HD:] = jnp.where(ok, 1.0, 0.0).astype(BF16)

    def unit(q, k, vx, h, acc, first, mode, offset):
        per = QT // chunk

        def tile(i, carry):
            span = pl.ds(pl.multiple_of(i * QT, QT), QT)
            qt = q[h, span]
            ps = []
            kb = 256
            if mode:
                shape = (per, n_tp, sub, kb)
                c0 = lax.rem(i * per, NC)
                pos = (
                    (c0 + lax.broadcasted_iota(jnp.int32, shape, 0)) * sub
                    + lax.broadcasted_iota(jnp.int32, shape, 1) * owned
                    + lax.broadcasted_iota(jnp.int32, shape, 2)
                )
                rel = (lax.broadcasted_iota(jnp.int32, shape, 3) - pos - offset).reshape(QT, kb)
            for b in range(ctx // kb):
                sc = lax.dot_general(
                    qt, k[h, b * kb:(b + 1) * kb], (((1,), (1,)), ((), ())),
                    preferred_element_type=F32)
                p = jnp.exp2(jnp.tanh(sc) * GAIN)
                if mode == 1:
                    p = jnp.where(rel <= -b * kb, p, 0.0)
                elif mode == 2:
                    p = jnp.where(rel > -b * kb, p, 0.0)
                ps.append(p.astype(BF16))
            a = jnp.dot(jnp.concatenate(ps, axis=1), vx[...], preferred_element_type=F32)
            if first:
                acc[h, span] = a
            else:
                acc[h, span] += a
            return carry

        lax.fori_loop(0, 2 * rows // QT, tile, 0, unroll=2)

    off_own = starts[s] - s * ctx
    s_next = jnp.minimum(s + 2, n - 1)
    off_next = starts[s_next] - s_next * ctx + (2 + 2) * ctx - WINDOW
    fill1 = counts[jnp.maximum(s - 1, 0)]
    fill2 = counts[jnp.maximum(s - 2, 0)]

    def own(h):
        for cp in kv_local(h):
            cp.wait()
        extend(vx0, v0, h, ctx)
        unit(qo, k0, vx0, h, ao, True, 1, off_own)

    def back(h):
        @pl.when(has_prev)
        def _():
            for cp in kv_next(h):
                cp.wait_recv()

        @pl.when(has_prev & (odd == 1))
        def _():
            for cp in kv_relay(h):
                cp.start()

        @pl.when(has_next)
        def _():
            q_back(h).wait_recv()
            ar[h] = jnp.zeros_like(ar[h])

        @pl.when(has_prev)
        def _():
            extend(vx2, v2, h, fill2)

            @pl.when(has_next)
            def _():
                unit(qr, k2, vx2, h, ar, False, 2, off_next)

        @pl.when(s >= 1)
        def _():
            for cp in kv_own_partner(h):
                cp.wait_recv()

            extend(vx1, v1, h, fill1)

            @pl.when(has_next)
            def _():
                unit(qr, k1, vx1, h, ar, False, 0, 0)

    def far(h):
        @pl.when(has_prev)
        def _():
            unit(qo, k2, vx2, h, ao, False, 0, 0)

        @pl.when(s >= 1)
        def _():
            unit(qo, k1, vx1, h, ao, False, 0, 0)

    own(0)

    def head(h, carry):
        back(h)

        @pl.when(h < kvh - 1)
        def _():
            far(h)
            own(h + 1)

        return carry

    lax.fori_loop(0, kvh, head, 0)

    lane = lax.broadcasted_iota(jnp.int32, (chunk, HD), 1)
    heads = 2 * kvh

    @pl.when(has_next)
    def _():
        for c in range(NC):
            pack = jnp.zeros((chunk, HD), F32)
            for h in range(kvh):
                for g in range(2):
                    r0 = g * rows + c * chunk
                    j = 2 * h + g
                    psend[c, j] = ar[h, r0:r0 + chunk, 0:HD].astype(BF16)
                    den = ar[h, r0:r0 + chunk, HD:2 * HD]
                    hi = den.astype(BF16).astype(F32)
                    pack = jnp.where(lane == j, hi, pack)
                    pack = jnp.where(lane == heads + j, den - hi, pack)
            psend[c, heads] = pack.astype(BF16)
            part_next(c).start()

    far(kvh - 1)
    wo_copy.wait()

    @pl.when(s < 2)
    def _():
        precv[...] = jnp.zeros_like(precv)

    def finish(c, carry):
        @pl.when(has_prev)
        def _():
            part_next(c).wait_recv()

        pack = precv[c, heads].astype(F32)
        for h in range(kvh):
            for g in range(2):
                j = 2 * h + g
                span = pl.ds(pl.multiple_of(g * rows + c * chunk, chunk), chunk)
                den = (
                    ao[h, span, HD:2 * HD]
                    + pack[:, j:j + 1] + pack[:, heads + j:heads + j + 1]
                )
                num = ao[h, span, 0:HD] + precv[c, j].astype(F32)
                att[:, j * HD:(j + 1) * HD] = (num / den).astype(BF16)

        def column(i, inner):
            cs = pl.ds(pl.multiple_of(i * NT, NT), NT)
            y = jnp.dot(att[...], wob[:, cs], preferred_element_type=F32).astype(BF16)
            proj[c, :, :, :, cs] = y.reshape(ny, nx, sub, NT)
            return inner

        lax.fori_loop(0, d // NT, column, 0)
        for cp in first_phase(c):
            cp.start()

        @pl.when(c >= 1)
        def _():
            middle(c - 1)

        return carry

    def middle(c):
        for cp in first_phase(c):
            cp.wait_recv()
        for y in range(ny):
            part = proj[c, y, x_own, :, 0:half].astype(F32)
            for k in range(1, nx):
                part += ra1[c, k - 1, y].astype(F32)
            pa[c, y] = part.astype(BF16)
        for x in range(nx):
            part = proj[c, y_own, x, :, half:d].astype(F32)
            for k in range(1, ny):
                part += rb1[c, k - 1, x].astype(F32)
            pb[c, x] = part.astype(BF16)
        for cp in second_phase(c):
            cp.start()

    lax.fori_loop(0, NC, finish, 0)
    middle(NC - 1)
    res_copy.wait()

    def out_copy(c):
        return pltpu.make_async_copy(
            obuf.at[c], out.at[pl.ds(pl.multiple_of(c * sub, sub), sub)], osem.at[c])

    def close(c, carry):
        for cp in second_phase(c):
            cp.wait_recv()
        lo = pa[c, y_own].astype(F32)
        for k in range(1, ny):
            lo += ra2[c, k - 1].astype(F32)
        hi = pb[c, x_own].astype(F32)
        for k in range(1, nx):
            hi += rb2[c, k - 1].astype(F32)
        squares = jnp.sum(lo * lo, axis=-1, keepdims=True) + jnp.sum(hi * hi, axis=-1, keepdims=True)
        scale = lax.rsqrt(squares / d + 0.1)
        span = pl.ds(pl.multiple_of(c * sub, sub), sub)
        for v, at in ((lo, slice(0, half)), (hi, slice(half, d))):
            r = res[span, at].astype(F32)
            obuf[c, :, at] = (r + v * scale * post_gain[:, at]).astype(BF16)
        out_copy(c).start()
        return carry

    lax.fori_loop(0, NC, close, 0)

    def drain(h, carry):
        @pl.when(has_next)
        def _():
            for cp in kv_next(h):
                cp.wait_send()

        @pl.when(odd == 0)
        def _():
            for cp in kv_own_partner(h):
                cp.wait_send()

        @pl.when(has_prev & (odd == 1))
        def _():
            for cp in kv_relay(h):
                cp.wait_send()

        @pl.when(has_prev)
        def _():
            q_back(h).wait_send()

        return carry

    lax.fori_loop(0, kvh, drain, 0)

    def drain_chunks(c, carry):
        @pl.when(has_next)
        def _():
            part_next(c).wait_send()

        for cp in first_phase(c) + second_phase(c):
            cp.wait_send()
        out_copy(c).wait()
        return carry

    lax.fori_loop(0, NC, drain_chunks, 0)


def shards(n, n_tp, hidden_in, pre_gain, w_query, key_cache, value_cache, w_out, post_gain, starts, counts):
    rows, d = hidden_in.shape
    ctx, kvw = key_cache.shape
    kvh = kvw // HD
    sub = SUB
    NC = rows // (n_tp * sub)
    chunk = rows // NC
    nx, ny, half = 2, n_tp // 2, d // 2
    dma = pltpu.SemaphoreType.DMA
    kv = pltpu.VMEM((kvh, ctx, HD), BF16)
    any_spec = pl.BlockSpec(memory_space=pl.ANY)
    vmem_spec = pl.BlockSpec(memory_space=pltpu.VMEM)
    smem_spec = pl.BlockSpec(memory_space=pltpu.SMEM)
    return pl.pallas_call(
        functools.partial(kernel, n, n_tp, kvh, NC),
        out_shape=jax.ShapeDtypeStruct((rows // n_tp, d), BF16),
        in_specs=[smem_spec, smem_spec, any_spec, vmem_spec] + [any_spec] * 4 + [vmem_spec],
        out_specs=any_spec,
        scratch_shapes=[
            pltpu.VMEM((NC, n_tp, sub, d), BF16),
            pltpu.VMEM((kvh, d, 2 * HD), BF16),
            pltpu.VMEM(w_out.shape, BF16),
            kv, kv, kv, kv, kv, kv,
            pltpu.VMEM((kvh, 2 * rows, HD), BF16),
            pltpu.VMEM((kvh, 2 * rows, HD), BF16),
            pltpu.VMEM((ctx, 2 * HD), BF16),
            pltpu.VMEM((ctx, 2 * HD), BF16),
            pltpu.VMEM((ctx, 2 * HD), BF16),
            pltpu.VMEM((kvh, 2 * rows, 2 * HD), F32),
            pltpu.VMEM((kvh, 2 * rows, 2 * HD), F32),
            pltpu.VMEM((NC, 2 * kvh + 1, chunk, HD), BF16),
            pltpu.VMEM((NC, 2 * kvh + 1, chunk, HD), BF16),
            pltpu.VMEM((NC, ny, nx, sub, d), BF16),
            pltpu.VMEM((NC, nx - 1, ny, sub, half), BF16),
            pltpu.VMEM((NC, ny, sub, half), BF16),
            pltpu.VMEM((NC, ny - 1, sub, half), BF16),
            pltpu.VMEM((NC, ny - 1, nx, sub, half), BF16),
            pltpu.VMEM((NC, nx, sub, half), BF16),
            pltpu.VMEM((NC, nx - 1, sub, half), BF16),
            pltpu.VMEM((rows // n_tp, d), BF16),
            pltpu.VMEM((NC, sub, d), BF16),
            pltpu.VMEM((chunk, w_out.shape[0]), BF16),
            dma((NC, n_tp)), dma((kvh,)), dma, dma((kvh, 2)), dma, dma((NC,)),
            dma((kvh, 2)), dma((kvh, 2)), dma((kvh, 2)), dma((kvh, 2)),
            dma((kvh,)), dma((kvh,)), dma((NC,)), dma((NC,)),
            dma((NC, nx - 1)), dma((NC, nx - 1)), dma((NC, ny - 1)), dma((NC, ny - 1)),
            dma((NC, ny - 1)), dma((NC, ny - 1)), dma((NC, nx - 1)), dma((NC, nx - 1)),
        ],
        compiler_params=pltpu.CompilerParams(
            collective_id=0, has_side_effects=True, vmem_limit_bytes=67_000_000),
        name="attention_block",
    )(starts, counts, hidden_in, pre_gain.reshape(1, d), w_query, key_cache, value_cache, w_out,
      post_gain.reshape(1, d))


def solution(mesh):
    return jax.shard_map(
        functools.partial(shards, mesh.shape["seq"], mesh.shape["tp"]),
        mesh=mesh,
        in_specs=(
            P("seq", None),
            P(),
            P(None, "tp"),
            P("seq", "tp"),
            P("seq", "tp"),
            P("tp", None),
            P(),
            P(),
            P(),
        ),
        out_specs=P(("seq", "tp"), None),
        check_vma=False,
    )
```

```python
import functools
import math

import jax
import jax.numpy as jnp
from jax import lax
from jax.experimental import pallas as pl
from jax.experimental.pallas import tpu as pltpu
from jax.sharding import PartitionSpec as P

HEADS = 32
HD = 128
WINDOW = 4096
SUB = 16
QT = 256
NT = 256
SOFT = 50.0
GAIN = SOFT * math.log2(math.e)
MESH = pl.DeviceIdType.MESH
F32 = jnp.float32
BF16 = jnp.bfloat16


def kernel(
    n, n_tp, kvh, NC,
    starts, counts, hidden, pre_gain, wq, key, value, wout, post_gain, out,
    hbuf, wqb, wob, k0, v0, k2, v2, k1, v1, qo, qr, vx0, vx1, vx2, ao, ar, psend, precv,
    proj, ra1, pa, ra2, rb1, pb, rb2, res, obuf, att,
    hsem, wqsem, wosem, kvsem, ressem, osem,
    s2, r2, s1, r1, sq, rq, sp, rp,
    sa1, ta1, sa2, ta2, sb1, tb1, sb2, tb2,
):
    s = lax.axis_index("seq")
    t = lax.axis_index("tp")
    odd = lax.rem(s, 2)
    partner = s + 1 - 2 * odd
    rows, d = hidden.shape
    ctx = key.shape[0]
    sub = rows // (NC * n_tp)
    chunk = rows // NC
    owned = rows // n_tp
    has_prev = s >= 2
    has_next = s + 2 < n

    hcopies = []
    for c in range(NC):
        for b in range(n_tp):
            cp = pltpu.make_async_copy(
                hidden.at[pl.ds(b * owned + c * sub, sub)], hbuf.at[c, b], hsem.at[c, b])
            cp.start()
            hcopies.append(cp)

    def wq_copy(h):
        return pltpu.make_async_copy(
            wq.at[:, pl.ds(pl.multiple_of(h * 2 * HD, 2 * HD), 2 * HD)], wqb.at[h], wqsem.at[h])

    for h in range(kvh):
        wq_copy(h).start()

    barrier = pltpu.get_barrier_semaphore()
    pl.semaphore_signal(barrier, inc=1, device_id=(partner, t), device_id_type=MESH)
    for k in range(1, n_tp):
        pl.semaphore_signal(barrier, inc=1, device_id=(s, lax.rem(t + k, n_tp)), device_id_type=MESH)

    @pl.when(has_prev)
    def _():
        pl.semaphore_signal(barrier, inc=1, device_id=(s - 2, t), device_id_type=MESH)

    @pl.when(has_next)
    def _():
        pl.semaphore_signal(barrier, inc=1, device_id=(s + 2, t), device_id_type=MESH)

    pl.semaphore_wait(
        barrier, n_tp + jnp.where(has_prev, 1, 0) + jnp.where(has_next, 1, 0))

    def cols(h):
        return pl.ds(pl.multiple_of(h * HD, HD), HD)

    def kv_next(h):
        return [
            pltpu.make_async_remote_copy(
                src.at[:, cols(h)], dst.at[h], s2.at[h, j], r2.at[h, j],
                device_id=(s + 2, t), device_id_type=MESH)
            for j, (src, dst) in enumerate(((key, k2), (value, v2)))
        ]

    def kv_own_partner(h):
        return [
            pltpu.make_async_remote_copy(
                src.at[:, cols(h)], dst.at[h], s1.at[h, j], r1.at[h, j],
                device_id=(partner, t), device_id_type=MESH)
            for j, (src, dst) in enumerate(((key, k1), (value, v1)))
        ]

    def kv_relay(h):
        return [
            pltpu.make_async_remote_copy(
                src.at[h], dst.at[h], s1.at[h, j], r1.at[h, j],
                device_id=(partner, t), device_id_type=MESH)
            for j, (src, dst) in enumerate(((k2, k1), (v2, v1)))
        ]

    def q_back(h):
        return pltpu.make_async_remote_copy(
            qo.at[h], qr.at[h], sq.at[h], rq.at[h], device_id=(s - 2, t), device_id_type=MESH)

    def part_next(c):
        return pltpu.make_async_remote_copy(
            psend.at[c], precv.at[c], sp.at[c], rp.at[c],
            device_id=(s + 2, t), device_id_type=MESH)

    nx = 2
    ny = n_tp // nx
    half = d // 2
    x_own = lax.rem(t, nx)
    y_own = lax.div(t, nx)
    left = pl.ds(0, half)
    right = pl.ds(half, half)

    def remote(src, dst, send, recv, to):
        return pltpu.make_async_remote_copy(
            src, dst, send, recv, device_id=(s, to), device_id_type=MESH)

    def first_phase(c):
        copies = []
        for k in range(1, nx):
            xt = lax.rem(x_own + k, nx)
            copies.append(remote(
                proj.at[c, :, xt, :, left], ra1.at[c, k - 1], sa1.at[c, k - 1], ta1.at[c, k - 1],
                y_own * nx + xt))
        for k in range(1, ny):
            yt = lax.rem(y_own + k, ny)
            copies.append(remote(
                proj.at[c, yt, :, :, right], rb1.at[c, k - 1], sb1.at[c, k - 1], tb1.at[c, k - 1],
                yt * nx + x_own))
        return copies

    def second_phase(c):
        copies = []
        for k in range(1, ny):
            yt = lax.rem(y_own + k, ny)
            copies.append(remote(
                pa.at[c, yt], ra2.at[c, k - 1], sa2.at[c, k - 1], ta2.at[c, k - 1],
                yt * nx + x_own))
        for k in range(1, nx):
            xt = lax.rem(x_own + k, nx)
            copies.append(remote(
                pb.at[c, xt], rb2.at[c, k - 1], sb2.at[c, k - 1], tb2.at[c, k - 1],
                y_own * nx + xt))
        return copies

    @pl.when(has_next)
    def _():
        for h in range(kvh):
            for cp in kv_next(h):
                cp.start()

    @pl.when(odd == 0)
    def _():
        for h in range(kvh):
            for cp in kv_own_partner(h):
                cp.start()

    def kv_local(h):
        return [
            pltpu.make_async_copy(src.at[:, cols(h)], dst.at[h], kvsem.at[h, j])
            for j, (src, dst) in enumerate(((key, k0), (value, v0)))
        ]

    for h in range(kvh):
        for cp in kv_local(h):
            cp.start()
    wo_copy = pltpu.make_async_copy(wout, wob, wosem)
    wo_copy.start()
    res_copy = pltpu.make_async_copy(
        hidden.at[pl.ds(pl.multiple_of(t * owned, owned), owned)], res, ressem)
    res_copy.start()

    for cp in hcopies:
        cp.wait()

    def norm(i, carry):
        c = i // n_tp
        b = i % n_tp
        x = hbuf[c, b].astype(F32)
        y = x * lax.rsqrt(jnp.mean(x * x, axis=-1, keepdims=True) + 0.1) * pre_gain[...]
        hbuf[c, b] = y.astype(BF16)
        return carry

    lax.fori_loop(0, NC * n_tp, norm, 0)

    def project(h, carry):
        wq_copy(h).wait()
        x = hbuf[...].reshape(rows, d)
        y = jnp.dot(x, wqb[h], preferred_element_type=F32) * ((d // HEADS) ** -0.5 / SOFT)
        y = y.astype(BF16)
        qo[h, 0:rows] = y[:, :HD]
        qo[h, rows:2 * rows] = y[:, HD:]

        @pl.when(has_prev)
        def _():
            q_back(h).start()

        return carry

    lax.fori_loop(0, kvh, project, 0)

    def extend(vx, v, h, filled):
        r = lax.broadcasted_iota(jnp.int32, (ctx, HD), 0)
        ok = r < filled
        vx[:, 0:HD] = jnp.where(ok, v[h].astype(F32), 0.0).astype(BF16)
        vx[:, HD:] = jnp.where(ok, 1.0, 0.0).astype(BF16)

    def unit(q, k, vx, h, acc, first, mode, offset):
        per = QT // chunk

        def tile(i, carry):
            span = pl.ds(pl.multiple_of(i * QT, QT), QT)
            qt = q[h, span]
            ps = []
            kb = 256
            if mode:
                shape = (per, n_tp, sub, kb)
                c0 = lax.rem(i * per, NC)
                pos = (
                    (c0 + lax.broadcasted_iota(jnp.int32, shape, 0)) * sub
                    + lax.broadcasted_iota(jnp.int32, shape, 1) * owned
                    + lax.broadcasted_iota(jnp.int32, shape, 2)
                )
                rel = (lax.broadcasted_iota(jnp.int32, shape, 3) - pos - offset).reshape(QT, kb)
            for b in range(ctx // kb):
                sc = lax.dot_general(
                    qt, k[h, b * kb:(b + 1) * kb], (((1,), (1,)), ((), ())),
                    preferred_element_type=F32)
                p = jnp.exp2(jnp.tanh(sc) * GAIN)
                if mode == 1:
                    p = jnp.where(rel <= -b * kb, p, 0.0)
                elif mode == 2:
                    p = jnp.where(rel > -b * kb, p, 0.0)
                ps.append(p.astype(BF16))
            a = jnp.dot(jnp.concatenate(ps, axis=1), vx[...], preferred_element_type=F32)
            if first:
                acc[h, span] = a
            else:
                acc[h, span] += a
            return carry

        lax.fori_loop(0, 2 * rows // QT, tile, 0, unroll=2)

    off_own = starts[s] - s * ctx
    s_next = jnp.minimum(s + 2, n - 1)
    off_next = starts[s_next] - s_next * ctx + (2 + 2) * ctx - WINDOW
    fill1 = counts[jnp.maximum(s - 1, 0)]
    fill2 = counts[jnp.maximum(s - 2, 0)]

    def own(h):
        for cp in kv_local(h):
            cp.wait()
        extend(vx0, v0, h, ctx)
        unit(qo, k0, vx0, h, ao, True, 1, off_own)

    def back(h):
        @pl.when(has_prev)
        def _():
            for cp in kv_next(h):
                cp.wait_recv()

        @pl.when(has_prev & (odd == 1))
        def _():
            for cp in kv_relay(h):
                cp.start()

        @pl.when(has_next)
        def _():
            q_back(h).wait_recv()
            ar[h] = jnp.zeros_like(ar[h])

        @pl.when(has_prev)
        def _():
            extend(vx2, v2, h, fill2)

            @pl.when(has_next)
            def _():
                unit(qr, k2, vx2, h, ar, False, 2, off_next)

        @pl.when(s >= 1)
        def _():
            for cp in kv_own_partner(h):
                cp.wait_recv()

            extend(vx1, v1, h, fill1)

            @pl.when(has_next)
            def _():
                unit(qr, k1, vx1, h, ar, False, 0, 0)

    def far(h):
        @pl.when(has_prev)
        def _():
            unit(qo, k2, vx2, h, ao, False, 0, 0)

        @pl.when(s >= 1)
        def _():
            unit(qo, k1, vx1, h, ao, False, 0, 0)

    own(0)

    def head(h, carry):
        back(h)

        @pl.when(h < kvh - 1)
        def _():
            far(h)
            own(h + 1)

        return carry

    lax.fori_loop(0, kvh, head, 0)

    lane = lax.broadcasted_iota(jnp.int32, (chunk, HD), 1)
    heads = 2 * kvh

    @pl.when(has_next)
    def _():
        for c in range(NC):
            pack = jnp.zeros((chunk, HD), F32)
            for h in range(kvh):
                for g in range(2):
                    r0 = g * rows + c * chunk
                    j = 2 * h + g
                    psend[c, j] = ar[h, r0:r0 + chunk, 0:HD].astype(BF16)
                    den = ar[h, r0:r0 + chunk, HD:2 * HD]
                    hi = den.astype(BF16).astype(F32)
                    pack = jnp.where(lane == j, hi, pack)
                    pack = jnp.where(lane == heads + j, den - hi, pack)
            psend[c, heads] = pack.astype(BF16)
            part_next(c).start()

    far(kvh - 1)
    wo_copy.wait()

    @pl.when(s < 2)
    def _():
        precv[...] = jnp.zeros_like(precv)

    def finish(c, carry):
        @pl.when(has_prev)
        def _():
            part_next(c).wait_recv()

        pack = precv[c, heads].astype(F32)
        for h in range(kvh):
            for g in range(2):
                j = 2 * h + g
                span = pl.ds(pl.multiple_of(g * rows + c * chunk, chunk), chunk)
                den = (
                    ao[h, span, HD:2 * HD]
                    + pack[:, j:j + 1] + pack[:, heads + j:heads + j + 1]
                )
                num = ao[h, span, 0:HD] + precv[c, j].astype(F32)
                att[:, j * HD:(j + 1) * HD] = (num / den).astype(BF16)

        def column(i, inner):
            cs = pl.ds(pl.multiple_of(i * NT, NT), NT)
            y = jnp.dot(att[...], wob[:, cs], preferred_element_type=F32).astype(BF16)
            proj[c, :, :, :, cs] = y.reshape(ny, nx, sub, NT)
            return inner

        lax.fori_loop(0, d // NT, column, 0)
        for cp in first_phase(c):
            cp.start()

        @pl.when(c >= 1)
        def _():
            middle(c - 1)

        return carry

    def middle(c):
        for cp in first_phase(c):
            cp.wait_recv()
        for y in range(ny):
            part = proj[c, y, x_own, :, 0:half].astype(F32)
            for k in range(1, nx):
                part += ra1[c, k - 1, y].astype(F32)
            pa[c, y] = part.astype(BF16)
        for x in range(nx):
            part = proj[c, y_own, x, :, half:d].astype(F32)
            for k in range(1, ny):
                part += rb1[c, k - 1, x].astype(F32)
            pb[c, x] = part.astype(BF16)
        for cp in second_phase(c):
            cp.start()

    lax.fori_loop(0, NC, finish, 0)
    middle(NC - 1)
    res_copy.wait()

    def out_copy(c):
        return pltpu.make_async_copy(
            obuf.at[c], out.at[pl.ds(pl.multiple_of(c * sub, sub), sub)], osem.at[c])

    def close(c, carry):
        for cp in second_phase(c):
            cp.wait_recv()
        lo = pa[c, y_own].astype(F32)
        for k in range(1, ny):
            lo += ra2[c, k - 1].astype(F32)
        hi = pb[c, x_own].astype(F32)
        for k in range(1, nx):
            hi += rb2[c, k - 1].astype(F32)
        squares = jnp.sum(lo * lo, axis=-1, keepdims=True) + jnp.sum(hi * hi, axis=-1, keepdims=True)
        scale = lax.rsqrt(squares / d + 0.1)
        span = pl.ds(pl.multiple_of(c * sub, sub), sub)
        for v, at in ((lo, slice(0, half)), (hi, slice(half, d))):
            r = res[span, at].astype(F32)
            obuf[c, :, at] = (r + v * scale * post_gain[:, at]).astype(BF16)
        out_copy(c).start()
        return carry

    lax.fori_loop(0, NC, close, 0)

    def drain(h, carry):
        @pl.when(has_next)
        def _():
            for cp in kv_next(h):
                cp.wait_send()

        @pl.when(odd == 0)
        def _():
            for cp in kv_own_partner(h):
                cp.wait_send()

        @pl.when(has_prev & (odd == 1))
        def _():
            for cp in kv_relay(h):
                cp.wait_send()

        @pl.when(has_prev)
        def _():
            q_back(h).wait_send()

        return carry

    lax.fori_loop(0, kvh, drain, 0)

    def drain_chunks(c, carry):
        @pl.when(has_next)
        def _():
            part_next(c).wait_send()

        for cp in first_phase(c) + second_phase(c):
            cp.wait_send()
        out_copy(c).wait()
        return carry

    lax.fori_loop(0, NC, drain_chunks, 0)


def shards(n, n_tp, hidden_in, pre_gain, w_query, key_cache, value_cache, w_out, post_gain, starts, counts):
    rows, d = hidden_in.shape
    ctx, kvw = key_cache.shape
    kvh = kvw // HD
    sub = SUB
    NC = rows // (n_tp * sub)
    chunk = rows // NC
    nx, ny, half = 2, n_tp // 2, d // 2
    dma = pltpu.SemaphoreType.DMA
    kv = pltpu.VMEM((kvh, ctx, HD), BF16)
    any_spec = pl.BlockSpec(memory_space=pl.ANY)
    vmem_spec = pl.BlockSpec(memory_space=pltpu.VMEM)
    smem_spec = pl.BlockSpec(memory_space=pltpu.SMEM)
    return pl.pallas_call(
        functools.partial(kernel, n, n_tp, kvh, NC),
        out_shape=jax.ShapeDtypeStruct((rows // n_tp, d), BF16),
        in_specs=[smem_spec, smem_spec, any_spec, vmem_spec] + [any_spec] * 4 + [vmem_spec],
        out_specs=any_spec,
        scratch_shapes=[
            pltpu.VMEM((NC, n_tp, sub, d), BF16),
            pltpu.VMEM((kvh, d, 2 * HD), BF16),
            pltpu.VMEM(w_out.shape, BF16),
            kv, kv, kv, kv, kv, kv,
            pltpu.VMEM((kvh, 2 * rows, HD), BF16),
            pltpu.VMEM((kvh, 2 * rows, HD), BF16),
            pltpu.VMEM((ctx, 2 * HD), BF16),
            pltpu.VMEM((ctx, 2 * HD), BF16),
            pltpu.VMEM((ctx, 2 * HD), BF16),
            pltpu.VMEM((kvh, 2 * rows, 2 * HD), F32),
            pltpu.VMEM((kvh, 2 * rows, 2 * HD), F32),
            pltpu.VMEM((NC, 2 * kvh + 1, chunk, HD), BF16),
            pltpu.VMEM((NC, 2 * kvh + 1, chunk, HD), BF16),
            pltpu.VMEM((NC, ny, nx, sub, d), BF16),
            pltpu.VMEM((NC, nx - 1, ny, sub, half), BF16),
            pltpu.VMEM((NC, ny, sub, half), BF16),
            pltpu.VMEM((NC, ny - 1, sub, half), BF16),
            pltpu.VMEM((NC, ny - 1, nx, sub, half), BF16),
            pltpu.VMEM((NC, nx, sub, half), BF16),
            pltpu.VMEM((NC, nx - 1, sub, half), BF16),
            pltpu.VMEM((rows // n_tp, d), BF16),
            pltpu.VMEM((NC, sub, d), BF16),
            pltpu.VMEM((chunk, w_out.shape[0]), BF16),
            dma((NC, n_tp)), dma((kvh,)), dma, dma((kvh, 2)), dma, dma((NC,)),
            dma((kvh, 2)), dma((kvh, 2)), dma((kvh, 2)), dma((kvh, 2)),
            dma((kvh,)), dma((kvh,)), dma((NC,)), dma((NC,)),
            dma((NC, nx - 1)), dma((NC, nx - 1)), dma((NC, ny - 1)), dma((NC, ny - 1)),
            dma((NC, ny - 1)), dma((NC, ny - 1)), dma((NC, nx - 1)), dma((NC, nx - 1)),
        ],
        compiler_params=pltpu.CompilerParams(
            collective_id=0, has_side_effects=True, vmem_limit_bytes=67_000_000),
        name="attention_block",
    )(starts, counts, hidden_in, pre_gain.reshape(1, d), w_query, key_cache, value_cache, w_out,
      post_gain.reshape(1, d))


def solution(mesh):
    return jax.shard_map(
        functools.partial(shards, mesh.shape["seq"], mesh.shape["tp"]),
        mesh=mesh,
        in_specs=(
            P("seq", None),
            P(),
            P(None, "tp"),
            P("seq", "tp"),
            P("seq", "tp"),
            P("tp", None),
            P(),
            P(),
            P(),
        ),
        out_specs=P(("seq", "tp"), None),
        check_vma=False,
    )
```
